32 devices in a mesh: dp: 4 (over x, core), tensor: 8 (over z, y).
Axes of the slice: x: 2, y: 2, z: 4, core: 2. Of those that a mesh axis runs over, the one named last changes fastest.
Arguments:
- attn_ctx: bfloat16 [2048, 8192], P('dp', 'tensor'), may hold values from -6 to 6
- w_out: bfloat16 [8192, 8192], P('tensor'), may hold values from -0.09375 to 0.09375
- resid: bfloat16 [2048, 8192], P(('dp', 'tensor')), may hold values from -6 to 6
- teacher_gain: bfloat16 [8192], replicated, may hold values from 0.25 to 1.75
- dest_row: int32 [2048], replicated, may hold values from 0 to 2047, as said below
- student_in: bfloat16 [2048, 4096], P('dp', 'tensor'), may hold values from -6 to 6
- student_gain: bfloat16 [4096], replicated, may hold values from 0.25 to 1.75
- w_gate: bfloat16 [4096, 14336], P('dp', 'tensor'), may hold values from -0.09375 to 0.09375
- w_up: bfloat16 [4096, 14336], P('dp', 'tensor'), may hold values from -0.09375 to 0.09375
- w_down: bfloat16 [14336, 4096], P('tensor', 'dp'), may hold values from -0.0625 to 0.0625
- proj: bfloat16 [4096, 8192], P('dp', 'tensor'), may hold values from -0.09375 to 0.09375
Outputs:
- student_out: bfloat16 [2048, 4096], P('dp', 'tensor')
- row_loss: float32 [2048], P('dp')
- residue: float32 [2048, 8192], P('dp', 'tensor')
The draws below stay inside these ranges and needn't reach their ends.
Inputs may be any that keep to these rules, and one draw needn't show every extreme that they name: A permutation of the rows; of the 64 rows i in one aligned block of teacher rows, at most 32 have dest_row[i] in any one tile of 512 student rows, and some tile receives exactly 32 of them.
All inputs are finite; a program needn't handle non-finite values.
Results may differ from the reference program's by a relative error of at most 0.012.
Values may be sent and summed in bfloat16 or wider, within the bound.
A program may use at most 192 MiB of HBM per device.

```python
import jax
import jax.numpy as jnp
from jax import lax

HT = 8192
D = 4096
FF = 14336
TT = 512
TOKENS = 2048
N_DP = 4
N_TENSOR = 8


def draw_dest_row(key, part):
    rows_dev = TT // N_TENSOR
    mean_count = rows_dev // N_DP
    sources = N_DP * N_TENSOR
    keys = jax.random.split(jax.random.fold_in(key, 7), 5)
    amounts = jax.random.randint(keys[0], (N_DP // 2,), 0, mean_count + 1)
    amounts = amounts.at[0].set(mean_count)
    counts = jnp.stack([mean_count + amounts, mean_count - amounts], 1).reshape(N_DP)
    counts = counts[jax.random.permutation(keys[1], N_DP)]
    rotation = jax.random.permutation(keys[2], sources) % N_DP
    shifted = (jnp.arange(N_DP)[None, :] + rotation[:, None]) % N_DP
    per_source = counts[shifted]
    bounds = jnp.cumsum(per_source, 1)
    position = jnp.arange(rows_dev)
    labels = jnp.sum((position[None, :, None] >= bounds[:, None, :]).astype(jnp.int32), 2)
    orders = jax.vmap(lambda one_key: jax.random.permutation(one_key, rows_dev))(jax.random.split(keys[3], sources))
    labels = jnp.take_along_axis(labels, orders, 1).reshape(-1)
    onehot = (labels[:, None] == jnp.arange(N_DP)[None, :]).astype(jnp.int32)
    ranking = jnp.sum((jnp.cumsum(onehot, 0) - onehot) * onehot, 1)
    placing = jax.vmap(lambda one_key: jax.random.permutation(one_key, TT))(jax.random.split(keys[4], N_DP))
    return (labels * TT + placing[labels, ranking]).astype(jnp.int32)


def with_spikes(drawn, stream_key, source, target, parts, factor):
    def block_of(axis_at):
        return (jnp.arange(drawn.shape[axis_at]) // (drawn.shape[axis_at] // parts)).reshape((-1,) + (1,) * (drawn.ndim - 1 - axis_at))

    near = jax.random.permutation(stream_key, parts)[block_of(target)]
    far = (block_of(target) + parts // 2) % parts
    return jnp.where((block_of(source) == near) | (block_of(source) == far), factor * drawn, drawn)


def level_of(stream_key, shape, cuts, least, high):
    factor_of = 1.0
    for dim, blocks in cuts:
        heights = jax.random.uniform(jax.random.fold_in(jax.random.fold_in(stream_key, 6), dim), (blocks,), jnp.float32, least / len(cuts), high / len(cuts))
        factor_of = factor_of * jnp.repeat(jnp.exp(heights), shape[dim] // blocks).reshape((-1,) + (1,) * (len(shape) - 1 - dim))
    return factor_of


def scatter_about(own_key, extent, scale, bound, cuts=(), kind=jnp.bfloat16):
    values = jax.random.normal(own_key, extent, jnp.float32) * scale
    if len(cuts) > 0:
        values = level_of(own_key, extent, cuts, -0.22, 0.18) * values
    return jnp.clip(values, min=-bound, max=bound).astype(kind)


def gaussian_with(key, shape, width, bound, cuts, heavy, dtype=jnp.bfloat16):
    values = width * jax.random.normal(key, shape, jnp.float32)
    if cuts:
        values = values * level_of(key, shape, cuts, -0.22, 0.18)
    return jnp.clip(with_spikes(values, jax.random.fold_in(key, 3), *heavy), -bound, bound).astype(dtype)


def setup_inputs(seed: int = 0) -> dict:
    splits = jax.random.split(jax.random.key(seed), 12)
    attn_ctx = scatter_about(splits[0], (TOKENS, HT), 1.0, 6.0, ((0, 4), (1, 8)))
    w_out = gaussian_with(splits[1], (HT, HT), HT ** -0.5, 0.09375, ((0, 8),), (0, 1, 8, 2.0))
    resid = scatter_about(splits[2], (TOKENS, HT), 1.0, 6.0, ((0, 32),))
    teacher_gain = jnp.clip(1.0 + 0.15 * jax.random.normal(splits[3], (HT,), jnp.float32), 0.25, 1.75).astype(jnp.bfloat16)
    dest_row = draw_dest_row(jax.random.fold_in(splits[11], 71), 0)
    student_in = scatter_about(splits[5], (TOKENS, D), 1.0, 6.0, ((0, 4), (1, 8)))
    student_gain = jnp.clip(1.0 + 0.15 * jax.random.normal(splits[6], (D,), jnp.float32), 0.25, 1.75).astype(jnp.bfloat16)
    w_gate = scatter_about(splits[7], (D, FF), D ** -0.5, 0.09375, ((0, 4), (1, 8)))
    w_up = scatter_about(splits[8], (D, FF), D ** -0.5, 0.09375, ((0, 4), (1, 8)))
    w_down = gaussian_with(splits[9], (FF, D), FF ** -0.5, 0.0625, ((0, 8), (1, 4)), (0, 1, 8, 2.0))
    proj = scatter_about(splits[10], (D, HT), D ** -0.5, 0.09375, ((0, 4), (1, 8)))
    return dict(attn_ctx=attn_ctx, w_out=w_out, resid=resid, teacher_gain=teacher_gain, dest_row=dest_row, student_in=student_in, student_gain=student_gain, w_gate=w_gate, w_up=w_up, w_down=w_down, proj=proj)


def reference(attn_ctx, w_out, resid, teacher_gain, dest_row, student_in, student_gain, w_gate, w_up, w_down, proj):
    blocks_ctx = attn_ctx.reshape(TOKENS, N_TENSOR, HT // N_TENSOR).transpose(1, 0, 2)
    blocks_out = w_out.reshape(N_TENSOR, HT // N_TENSOR, HT)

    def add_term(running, pair):
        term = jnp.dot(pair[0], pair[1], preferred_element_type=jnp.float32)
        term = lax.optimization_barrier(term.astype(jnp.bfloat16)).astype(jnp.float32)
        return (running + term, None)
    attn_sum, unused = lax.scan(add_term, jnp.zeros((TOKENS, HT), jnp.float32), (blocks_ctx, blocks_out))
    teacher_hidden = resid.astype(jnp.float32) + attn_sum
    square_mean = lax.optimization_barrier(jnp.mean(teacher_hidden * teacher_hidden, axis=1, keepdims=True))
    teacher_final = (teacher_hidden * lax.rsqrt(square_mean + 1e-06) * teacher_gain.astype(jnp.float32)).astype(jnp.bfloat16)
    target = jnp.zeros((TOKENS, HT), jnp.bfloat16).at[dest_row].set(teacher_final)
    x_full = student_in.astype(jnp.float32)
    student_mean = lax.optimization_barrier(jnp.mean(x_full * x_full, axis=1, keepdims=True))
    normed = (x_full * lax.rsqrt(student_mean + 1e-05) * student_gain.astype(jnp.float32)).astype(jnp.bfloat16)
    gate_acts = jnp.dot(normed, w_gate, preferred_element_type=jnp.float32)
    up_acts = jnp.dot(normed, w_up, preferred_element_type=jnp.float32)
    hidden = (jax.nn.silu(gate_acts) * up_acts).astype(jnp.bfloat16)
    mlp_sum = jnp.dot(hidden, w_down, preferred_element_type=jnp.float32)
    student_out = (x_full + mlp_sum).astype(jnp.bfloat16)
    pred = jnp.dot(student_out, proj, preferred_element_type=jnp.float32)
    residue = pred - target.astype(jnp.float32)
    row_loss = lax.optimization_barrier(jnp.mean(residue * residue, axis=1))
    return (student_out, row_loss, residue)
```

```python
import functools

import jax
import jax.numpy as jnp
from jax import lax
from jax.experimental import pallas as pl
from jax.experimental.pallas import tpu as pltpu
from jax.sharding import PartitionSpec as P

F32 = jnp.float32
BF16 = jnp.bfloat16
CORES = 2
MESH = pl.DeviceIdType.MESH
ANY = pl.BlockSpec(memory_space=pl.ANY)
VMEM = pl.BlockSpec(memory_space=pltpu.VMEM)
GRANT = 60 * 1024 * 1024


class Place:
    def __init__(self):
        self.n_dp = lax.axis_size("dp")
        self.n_t = lax.axis_size("tensor")
        self.n_x = self.n_dp // CORES
        self.n_y = self.n_x if self.n_t % self.n_x == 0 else 1
        self.n_z = self.n_t // self.n_y
        self.far = self.n_t // 2
        self.dp = lax.axis_index("dp")
        self.t = lax.axis_index("tensor")
        self.x = lax.div(self.dp, CORES)
        self.core = lax.rem(self.dp, CORES)
        self.spot = self.spot_of(self.t)
        self.sibling = self.x * CORES + 1 - self.core

    def spot_of(self, t):
        n_y, n_z = self.n_y, self.n_z
        if n_y == 1:
            return t
        z, y = lax.div(t, n_y), lax.rem(t, n_y)
        on = lax.div(y + n_y - 1, n_y)
        r = n_z - 1 - z
        i = y - 1 + lax.rem(r, 2) * (n_y - 2 * y)
        return (1 - on) * z + on * (n_z + r * (n_y - 1) + i)

    def at(self, offset):
        n_y, n_z = self.n_y, self.n_z
        p = lax.rem(self.spot + (offset + self.n_t), self.n_t)
        if n_y == 1:
            return p
        on = lax.div(lax.div(p, n_z) + n_y - 1, n_y)
        q = on * (p - n_z)
        r, i = lax.div(q, n_y - 1), lax.rem(q, n_y - 1)
        z = (1 - on) * p + on * (n_z - 1 - r)
        y = on * (1 + i + lax.rem(r, 2) * (n_y - 2 - 2 * i))
        return z * n_y + y

    def x_at(self, s):
        return lax.rem(self.x + s, self.n_x)

    def peer(self, s):
        return self.x_at(s) * CORES + self.core


def greet(devices):
    barrier = pltpu.get_barrier_semaphore()
    for device in devices:
        pl.semaphore_signal(barrier, inc=1, device_id=device, device_id_type=MESH)
    pl.semaphore_wait(barrier, len(devices))


def push(src, dst, send, recv, device):
    return pltpu.make_async_remote_copy(
        src_ref=src, dst_ref=dst, send_sem=send, recv_sem=recv, device_id=device, device_id_type=MESH
    )


def column_part(w, parts):
    cols = w.shape[1] // parts
    if cols % 128 == 0:
        return w
    return w.reshape(w.shape[0], parts, cols).transpose(1, 0, 2)


def part_of(ref, at, cols):
    if len(ref.shape) == 3:
        return ref.at[at]
    return ref.at[:, pl.ds(pl.multiple_of(at * cols, cols), cols)]


def gather_kernel(
    cols, rows_in, gate, up, down, x_all, gates, ups, downs,
    own_sem, ring_send, ring_recv, x_send, x_recv, core_send, core_recv,
):
    me = Place()
    n_x, far = me.n_x, me.far
    half = rows_in.shape[0] // 2
    line = [(me.dp, me.at(1)), (me.dp, me.at(-1))]
    peers = [(me.peer(s), me.t) for s in range(1, n_x)]
    twin = (me.sibling, me.t)
    greet(line + peers + [twin])

    own = pltpu.make_async_copy(rows_in, x_all.at[me.t, me.x], own_sem)
    own.start()

    def ring(k, d, s):
        t = me.at((1 - k) * (1 - 2 * d))
        dst = x_all.at[t, me.x_at(s)]
        src = rows_in if k == 1 and s == 0 else dst
        if k == far:
            rows = pl.ds(d * half, half)
            src, dst = src.at[rows], dst.at[rows]
        at = (d, k - 1, s)
        return push(src, dst, ring_send.at[at], ring_recv.at[at], line[d])

    started = []

    def start(copy):
        copy.start()
        started.append(copy)
        return copy

    hops = {}
    for d in range(2):
        hops[1, d, 0] = start(ring(1, d, 0))
    cross = [
        start(push(rows_in, x_all.at[me.t, me.x], x_send.at[0, s - 1], x_recv.at[0, s - 1], peers[s - 1]))
        for s in range(1, n_x)
    ]
    moved = {}
    for i, (w, buf) in enumerate(((gate, gates), (up, ups)), 1):
        for s in range(1, n_x):
            moved[i, s] = start(
                push(part_of(w, me.x_at(s), cols), buf.at[me.dp], x_send.at[i, s - 1], x_recv.at[i, s - 1], peers[s - 1])
            )
    twins = [
        start(push(part_of(gate, me.x, cols), gates.at[me.dp], core_send.at[0, 0], core_recv.at[0, 0], twin)),
        start(push(part_of(up, me.x, cols), ups.at[me.dp], core_send.at[1, 0], core_recv.at[1, 0], twin)),
        start(push(down, downs, core_send.at[2, 0], core_recv.at[2, 0], twin)),
    ]
    for s in range(1, n_x):
        cross[n_x - s - 1].wait_recv()
        for d in range(2):
            hops[1, d, s] = start(ring(1, d, s))

    def relay(i):
        buf = (gates, ups)[i - 1]
        for s in range(1, n_x):
            moved[i, s].wait_recv()
            block = buf.at[me.peer(n_x - s)]
            twins.append(start(push(block, block, core_send.at[i - 1, s], core_recv.at[i - 1, s], twin)))

    for k in range(1, far):
        for s in range(n_x):
            for d in range(2):
                hops[k, d, s].wait_recv()
                hops[k + 1, d, s] = start(ring(k + 1, d, s))
        if k == far - 2:
            relay(1)
    for s in range(n_x):
        for d in range(2):
            hops[far, d, s].wait_recv()
    if far < 3:
        relay(1)
    relay(2)
    for copy in twins:
        copy.wait_recv()
    own.wait()
    for copy in started:
        copy.wait_send()


def gather_rows(student_in, w_gate, w_up, w_down):
    n_dp, n_t = lax.axis_size("dp"), lax.axis_size("tensor")
    n_x = n_dp // CORES
    depth, cols = w_gate.shape[0], w_gate.shape[1] // n_x
    buf = jax.ShapeDtypeStruct((n_dp, depth, cols), BF16)
    sems = pltpu.SemaphoreType.DMA
    return pl.pallas_call(
        functools.partial(gather_kernel, cols),
        out_shape=(
            jax.ShapeDtypeStruct((n_t, n_x) + student_in.shape, BF16),
            buf,
            buf,
            jax.ShapeDtypeStruct(w_down.shape, BF16),
        ),
        in_specs=[VMEM, ANY, ANY, ANY],
        out_specs=(ANY,) * 4,
        scratch_shapes=[
            sems(()),
            sems((2, n_t // 2, n_x)),
            sems((2, n_t // 2, n_x)),
            sems((3, n_x)),
            sems((3, n_x)),
            sems((3, n_x)),
            sems((3, n_x)),
        ],
        compiler_params=pltpu.CompilerParams(collective_id=0, has_side_effects=True, vmem_limit_bytes=GRANT),
        name="gather_rows",
    )(student_in, column_part(w_gate, n_x), column_part(w_up, n_x), w_down)


def gated_kernel(cols, gain, x_all, gate, up, gates, ups, out, x_v, g_v, u_v, g_sum, u_sum, squares, x_sem, g_sem, u_sem):
    me = Place()
    n_x, n_dp, n_t = me.n_x, me.n_dp, me.n_t
    per = n_t // n_dp
    tokens, width = x_all.shape[2], x_all.shape[3]
    rows = n_x * tokens
    for i in range(n_dp):
        for own, buf, dst, sem in ((gate, gates, g_v, g_sem), (up, ups, u_v, u_sem)):

            @pl.when(me.dp == i)
            def _():
                pltpu.make_async_copy(part_of(own, me.x, cols), dst.at[i], sem.at[i]).start()

            @pl.when(me.dp != i)
            def _():
                pltpu.make_async_copy(buf.at[i], dst.at[i], sem.at[i]).start()

        for j in range(per):
            for x in range(n_x):
                pltpu.make_async_copy(
                    x_all.at[i * per + j, x],
                    x_v.at[i, pl.ds(x * tokens, tokens), pl.ds(j * width, width)],
                    x_sem.at[i, j, x],
                ).start()
    tile = min(256, rows)
    for i in range(n_dp):
        for j in range(per):
            for x in range(n_x):
                pltpu.make_async_copy(
                    x_all.at[i * per + j, x],
                    x_v.at[i, pl.ds(x * tokens, tokens), pl.ds(j * width, width)],
                    x_sem.at[i, j, x],
                ).wait()
        pltpu.make_async_copy(gates.at[i], g_v.at[i], g_sem.at[i]).wait()
        pltpu.make_async_copy(ups.at[i], u_v.at[i], u_sem.at[i]).wait()
        weight = gain[:, i * per * width : (i + 1) * per * width].astype(F32)

        @pl.loop(0, rows // tile)
        def _(r):
            at = pl.ds(pl.multiple_of(r * tile, tile), tile)
            x = x_v[i, at, :].astype(F32)
            square = jnp.sum(x * x, axis=1, keepdims=True)
            scaled = (x * weight).astype(BF16)
            g = jnp.dot(scaled, g_v[i], preferred_element_type=F32)
            u = jnp.dot(scaled, u_v[i], preferred_element_type=F32)
            if i:
                square = square + squares[at, :]
                g = g + g_sum[at, :]
                u = u + u_sum[at, :]
            if i < n_dp - 1:
                squares[at, :] = square
                g_sum[at, :] = g
                u_sum[at, :] = u
            else:
                scale = lax.rsqrt(square / (n_t * width) + 1e-05)
                g = g * scale
                out[at, :] = (jax.nn.silu(g) * (u * scale)).astype(BF16)


def gated(student_gain, x_all, w_gate, w_up, gates, ups):
    n_dp, depth, cols = gates.shape
    n_t, n_x, tokens, width = x_all.shape
    per = n_t // n_dp
    rows = n_x * tokens
    sems = pltpu.SemaphoreType.DMA
    flops = 4 * rows * n_dp * depth * cols
    return pl.pallas_call(
        functools.partial(gated_kernel, cols),
        out_shape=jax.ShapeDtypeStruct((rows, cols), BF16),
        in_specs=[VMEM] + [ANY] * 5,
        out_specs=VMEM,
        scratch_shapes=[
            pltpu.VMEM((n_dp, rows, per * width), BF16),
            pltpu.VMEM((n_dp, depth, cols), BF16),
            pltpu.VMEM((n_dp, depth, cols), BF16),
            pltpu.VMEM((rows, cols), F32),
            pltpu.VMEM((rows, cols), F32),
            pltpu.VMEM((rows, 1), F32),
            sems((n_dp, per, n_x)),
            sems((n_dp,)),
            sems((n_dp,)),
        ],
        compiler_params=pltpu.CompilerParams(vmem_limit_bytes=GRANT),
        cost_estimate=pl.CostEstimate(flops=flops, bytes_accessed=23_000_000, transcendentals=0),
        name="gated",
    )(student_gain[None, :], x_all, column_part(w_gate, n_x), column_part(w_up, n_x), gates, ups)


def as_row(column):
    return jnp.transpose(jnp.broadcast_to(column, (column.shape[0], 128)))[:8]


def as_column(row):
    return jnp.transpose(jnp.broadcast_to(row[:1], (128, row.shape[1])))[:, :1]


def add_over(peers, own, got, send, recv):
    copies = [push(own, got.at[k], send.at[k], recv.at[k], peer) for k, peer in enumerate(peers)]
    for copy in copies:
        copy.start()
    total = own[...]
    for k, copy in enumerate(copies):
        copy.wait_recv()
        total = total + got[k]
    for copy in copies:
        copy.wait_send()
    return total


def teacher_kernel(
    ctx, resid, gain, hidden, w_out, proj, out, hiddens, projs,
    w_v, sums, sent, got, total, row, rows_got,
    w_sem, send, recv, x_send, x_recv, core_send, core_recv, row_send, row_recv,
):
    me = Place()
    n_t, far = me.n_t, me.far
    width = w_v.shape[2]
    half = ctx.shape[0] // 2
    own = resid.shape[0]
    line = [(me.dp, me.at(1)), (me.dp, me.at(-1))]
    order = [far]
    for k in range(far - 1, 0, -1):
        order += [k, -k]
    order += [0]
    slot = {k: i for i, k in enumerate(order)}

    def load(k):
        cols = pl.ds(pl.multiple_of(me.at(k) * width, width), width)
        return pltpu.make_async_copy(w_out.at[:, cols], w_v.at[slot[k]], w_sem.at[slot[k]])

    for k in order:
        load(k).start()
    peers = [(me.peer(s), me.t) for s in range(1, me.n_x)]
    twin = (me.sibling, me.t)
    plane = [(me.dp, lax.rem(me.t + k, n_t)) for k in range(1, n_t)]
    greet(plane + peers + [twin])
    shared = []
    for s, peer in enumerate(peers):
        shared.append(push(hidden, hiddens.at[me.x], x_send.at[0, s], x_recv.at[0, s], peer))
    for s, peer in enumerate(peers):
        shared.append(push(proj, projs.at[me.dp], x_send.at[1, s], x_recv.at[1, s], peer))
    shared.append(push(proj, projs.at[me.dp], core_send.at[0], core_recv.at[0], twin))
    for copy in shared:
        copy.start()
    tile = min(256, width)

    def term(k, u):
        @pl.loop(0, width // tile)
        def _(c):
            cols = pl.ds(pl.multiple_of(c * tile, tile), tile)
            sums[:, cols] = jnp.dot(
                ctx[u * half : (u + 1) * half, :], w_v[slot[k], :, cols], preferred_element_type=F32
            )

        first = me.t * own

        @pl.when(lax.div(first, half) == u)
        def _():
            rows = pl.ds(pl.multiple_of(first - u * half, own), own)
            cols = pl.ds(pl.multiple_of(me.at(k) * width, width), width)
            sums[rows, :] = sums[rows, :] + resid[:, cols].astype(F32)

    def hop(k, d, u):
        at = (d, k - 1, u)
        return push(sent.at[at], got.at[at], send.at[at], recv.at[at], line[d])

    load(far).wait()
    for d in range(2):
        term(far, d)
        sent[d, far - 1, d] = sums[...].astype(BF16)
        hop(far, d, d).start()
    for k in range(far - 1, 0, -1):
        for d in range(2):
            load(k if d == 0 else -k).wait()
        for i in range(2):
            for d in range(2):
                u = (d + i + (k == far - 1)) % 2
                term(k if d == 0 else -k, u)
                if k + 1 < far or u == d:
                    hop(k + 1, d, u).wait_recv()
                    sent[d, k - 1, u] = (sums[...] + got[d, k, u].astype(F32)).astype(BF16)
                else:
                    sent[d, k - 1, u] = sums[...].astype(BF16)
                hop(k, d, u).start()
    load(0).wait()
    for i in range(2):
        term(0, i)
        for d in range(2):
            hop(1, d, i).wait_recv()
        total[i * half : (i + 1) * half, :] = (
            sums[...] + got[0, 0, i].astype(F32) + got[1, 0, i].astype(F32)
        )
    row[...] = as_row(jnp.sum(total[...] * total[...], axis=1, keepdims=True))
    for s in range(1, me.n_x):
        shared[me.n_x - 2 + s].wait_recv()
        block = projs.at[me.peer(me.n_x - s)]
        copy = push(block, block, core_send.at[s], core_recv.at[s], twin)
        copy.start()
        shared.append(copy)
    squares = add_over(plane, row, rows_got, row_send, row_recv)
    scale = as_column(lax.rsqrt(squares / (n_t * width) + 1e-06))
    weight = gain[:, pl.ds(pl.multiple_of(me.t * width, width), width)].astype(F32)
    out[...] = (total[...] * scale * weight).astype(BF16)
    for i, copy in enumerate(shared):
        if not me.n_x - 1 <= i < 2 * (me.n_x - 1):
            copy.wait_recv()
        copy.wait_send()
    for d in range(2):
        hop(far, d, d).wait_send()
        for k in range(far - 1, 0, -1):
            for u in range(2):
                hop(k, d, u).wait_send()


def teacher(attn_ctx, resid, w_out, teacher_gain, hidden, proj):
    n_t, n_dp = lax.axis_size("tensor"), lax.axis_size("dp")
    n_x = n_dp // CORES
    tokens, depth = attn_ctx.shape
    width = w_out.shape[1] // n_t
    sems = pltpu.SemaphoreType.DMA
    units = (2, n_t // 2, 2)
    return pl.pallas_call(
        teacher_kernel,
        out_shape=(
            jax.ShapeDtypeStruct((tokens, width), BF16),
            jax.ShapeDtypeStruct((n_x,) + hidden.shape, BF16),
            jax.ShapeDtypeStruct((n_dp,) + proj.shape, BF16),
        ),
        in_specs=[VMEM, VMEM, VMEM, ANY, ANY, ANY],
        out_specs=(VMEM, ANY, ANY),
        scratch_shapes=[
            pltpu.VMEM((n_t, depth, width), BF16),
            pltpu.VMEM((tokens // 2, width), F32),
            pltpu.VMEM(units + (tokens // 2, width), BF16),
            pltpu.VMEM(units + (tokens // 2, width), BF16),
            pltpu.VMEM((tokens, width), F32),
            pltpu.VMEM((8, tokens), F32),
            pltpu.VMEM((n_t - 1, 8, tokens), F32),
            sems((n_t,)),
            sems(units),
            sems(units),
            sems((2, n_x)),
            sems((2, n_x)),
            sems((n_x,)),
            sems((n_x,)),
            sems((n_t - 1,)),
            sems((n_t - 1,)),
        ],
        compiler_params=pltpu.CompilerParams(collective_id=1, has_side_effects=True, vmem_limit_bytes=GRANT),
        name="teacher",
    )(attn_ctx, resid, teacher_gain[None, :], hidden, w_out, proj)


def student_kernel(
    final, dest, hid_own, hiddens, w_down, downs, proj, projs, x_all, out, residue, loss,
    d_v, h_v, p_v, fin, full, mixed, here, sent, got, sums, target, column, row, rows_got,
    d_sem, h_sem, p_sem, here_sem, send, recv, fin_send, fin_recv, twin_send, twin_recv,
    swap_send, swap_recv, ring_send, ring_recv, row_send, row_recv,
):
    me = Place()
    n_x, n_t, n_dp, far = me.n_x, me.n_t, me.n_dp, me.far
    cols = h_v.shape[2]
    unit, block = d_v.shape[2], full.shape[3]
    tokens = final.shape[0]
    per = n_t // n_x
    half = sums.shape[0] // 2
    line = [(me.dp, me.at(1)), (me.dp, me.at(-1))]
    peers = [(me.peer(s), me.t) for s in range(1, n_x)]
    twin = (me.sibling, me.t)
    plane = [(me.dp, lax.rem(me.t + k, n_t)) for k in range(1, n_t)]

    def either(mine, index, own, other, dst, sem):
        @pl.when(mine == index)
        def _():
            pltpu.make_async_copy(own, dst, sem).start()

        @pl.when(mine != index)
        def _():
            pltpu.make_async_copy(other, dst, sem).start()

    for x in range(n_x):
        either(me.x, x, hid_own, hiddens.at[x], h_v.at[x], h_sem.at[x])
    for u in range(CORES):
        either(me.core, u, w_down, downs, d_v.at[u], d_sem.at[u])
    mine_rows = pl.ds(pl.multiple_of(me.t * block, block), block)
    width = x_all.shape[3]
    heres = [
        pltpu.make_async_copy(
            x_all.at[me.x * per + j, x, mine_rows], here.at[x, :, pl.ds(j * width, width)], here_sem.at[x, j]
        )
        for x in range(n_x)
        for j in range(per)
    ]
    for copy in heres:
        copy.start()
    for i in range(n_dp):
        either(me.dp, i, proj, projs.at[i], p_v.at[i], p_sem.at[i])
    greet(plane + peers + [twin])
    finals = [
        push(final, fin.at[me.dp], fin_send.at[s], fin_recv.at[s], peer) for s, peer in enumerate(peers)
    ] + [push(final, fin.at[me.dp], twin_send.at[0], twin_recv.at[0], twin)]
    for copy in finals:
        copy.start()
    fin[me.dp] = final[...]
    column[...] = jnp.zeros_like(column)
    for x in range(n_x):
        pltpu.make_async_copy(hid_own, h_v.at[x], h_sem.at[x]).wait()

    tile = min(256, unit)

    def term(k, u):
        t = me.at(k)

        @pl.loop(0, unit // tile)
        def _(c):
            at = pl.ds(pl.multiple_of(c * tile, tile), tile)
            total = None
            for x in range(n_x):
                rows = [h_v[x, pl.ds(pl.multiple_of(y * tokens + t * block, block), block), :] for y in range(n_x)]
                piece = jnp.dot(
                    jnp.concatenate(rows, axis=0),
                    d_v[u, x * cols : (x + 1) * cols, at],
                    preferred_element_type=F32,
                )
                total = piece if total is None else total + piece
            sums[:, at] = total

    def hop(k, d, u):
        at = (d, k - 1, u)
        src, dst = sent.at[at], got.at[at]
        if k == far:
            src, dst = src.at[pl.ds(d * half, half)], dst.at[pl.ds(d * half, half)]
        return push(src, dst, send.at[at], recv.at[at], line[d])

    for u in range(CORES):
        pltpu.make_async_copy(w_down, d_v.at[u], d_sem.at[u]).wait()
        term(far, u)
        for d in range(2):
            rows = slice(d * half, (d + 1) * half)
            sent[d, far - 1, u, rows] = sums[rows].astype(BF16)
            hop(far, d, u).start()
    for k in range(far - 1, 0, -1):
        for u in range(CORES):
            for d in range(2):
                term(k if d == 0 else -k, u)
                hop(k + 1, d, u).wait_recv()
                if k + 1 == far:
                    rows, rest = (slice(d * half, (d + 1) * half), slice((1 - d) * half, (2 - d) * half))
                    sent[d, k - 1, u, rows] = (sums[rows] + got[d, k, u, rows].astype(F32)).astype(BF16)
                    sent[d, k - 1, u, rest] = sums[rest].astype(BF16)
                else:
                    sent[d, k - 1, u] = (sums[...] + got[d, k, u].astype(F32)).astype(BF16)
                hop(k, d, u).start()
    for copy in heres:
        copy.wait()
    swaps = []
    for u in range(CORES):
        term(0, u)
        for d in range(2):
            hop(1, d, u).wait_recv()
        mlp = sums[...] + got[0, 0, u].astype(F32) + got[1, 0, u].astype(F32)
        known = here[:, :, u * unit : (u + 1) * unit].astype(F32)
        mixed[u] = (known + mlp.reshape(n_x, block, unit)).astype(BF16)
        full[me.t, u, me.x] = mixed[u, me.x]
        for s, peer in enumerate(peers):
            at = (u, s)
            copy = push(mixed.at[u, me.x_at(s + 1)], full.at[me.t, u, me.x], swap_send.at[at], swap_recv.at[at], peer)
            copy.start()
            swaps.append(copy)

    for s in range(1, n_x):
        finals[s - 1].wait_recv()
        piece = fin.at[me.peer(n_x - s)]
        copy = push(piece, piece, twin_send.at[s], twin_recv.at[s], twin)
        copy.start()
        finals.append(copy)

    def ring(k, d, u):
        t = me.at((1 - k) * (1 - 2 * d))
        view = full.at[t, u]
        if k == far:
            view = full.at[t, u, :, pl.ds(d * (block // 2), block // 2)]
        at = (d, k - 1, u)
        return push(view, view, ring_send.at[at], ring_recv.at[at], line[d])

    for u in range(CORES):
        for s in range(n_x - 1):
            swaps[u * (n_x - 1) + s].wait_recv()
        for d in range(2):
            ring(1, d, u).start()

    for copy in finals[n_x - 1 :]:
        copy.wait_recv()
    strip = min(256, tokens)

    @pl.loop(0, tokens // strip)
    def _(r):
        first = pl.multiple_of(r * strip, strip)
        places = me.dp * tokens + first + lax.broadcasted_iota(jnp.int32, (strip, tokens), 0)
        total = None
        for i in range(n_dp):
            pick = (places == dest[:, i * tokens : (i + 1) * tokens]).astype(F32).astype(BF16)
            piece = jnp.dot(pick, fin[i], preferred_element_type=F32)
            total = piece if total is None else total + piece
        target[pl.ds(first, strip), :] = total

    for i in range(n_dp):
        pltpu.make_async_copy(proj, p_v.at[i], p_sem.at[i]).wait()
    p_tile = min(256, target.shape[1])

    def project(ts):
        @pl.loop(0, target.shape[1] // p_tile)
        def _(c):
            at = pl.ds(pl.multiple_of(c * p_tile, p_tile), p_tile)
            total = None
            for x in range(n_x):
                for u in range(CORES):
                    rows = jnp.concatenate([full[t, u, x] for t in ts], axis=0)
                    piece = jnp.dot(rows, p_v[x * CORES + u, :, at], preferred_element_type=F32)
                    total = piece if total is None else total + piece
            for i, t in enumerate(ts):
                rows = pl.ds(pl.multiple_of(t * block, block), block)
                gap = total[i * block : (i + 1) * block] - target[rows, at]
                residue[rows, at] = gap
                column[rows, :] = column[rows, :] + jnp.sum(gap * gap, axis=1, keepdims=True)

    project([me.t])
    for k in range(1, far + 1):
        for u in range(CORES):
            for d in range(2):
                ring(k, d, u).wait_recv()
                if k < far:
                    ring(k + 1, d, u).start()
        project([me.at(-k), me.at(k)] if k < far else [me.at(far)])

    row[...] = as_row(column[...])
    out_cols = out.shape[1]
    x = lax.div(me.t, per)
    u = lax.div(lax.rem(me.t, per) * out_cols, unit)
    inner = pl.multiple_of(lax.rem(me.t * out_cols, unit), out_cols)
    for t in range(n_t):
        out[t * block : (t + 1) * block, :] = full[t, u, x, :, pl.ds(inner, out_cols)]
    loss[...] = add_over(plane, row, rows_got, row_send, row_recv) / (n_t * target.shape[1])
    for u in range(CORES):
        for d in range(2):
            for k in range(1, far + 1):
                hop(k, d, u).wait_send()
                ring(k, d, u).wait_send()
    for copy in finals + swaps:
        copy.wait_send()


def student(final, dest_row, hidden, hiddens, w_down, downs, proj, projs, x_all):
    n_t, n_dp = lax.axis_size("tensor"), lax.axis_size("dp")
    n_x, far = n_dp // CORES, n_t // 2
    tokens, width = final.shape
    ff, unit = w_down.shape
    rows, cols = hidden.shape
    block = tokens // n_t
    d_cols = x_all.shape[3]
    sems = pltpu.SemaphoreType.DMA
    hops = (2, far, CORES)
    vmem = pltpu.VMEM
    return pl.pallas_call(
        student_kernel,
        out_shape=(
            jax.ShapeDtypeStruct((tokens, d_cols), BF16),
            jax.ShapeDtypeStruct((tokens, width), F32),
            jax.ShapeDtypeStruct((8, tokens), F32),
        ),
        in_specs=[VMEM, VMEM] + [ANY] * 7,
        out_specs=(VMEM, VMEM, VMEM),
        scratch_shapes=[
            vmem((CORES, ff, unit), BF16),
            vmem((n_x, rows, cols), BF16),
            vmem((n_dp,) + proj.shape, BF16),
            vmem((n_dp, tokens, width), BF16),
            vmem((n_t, CORES, n_x, block, unit), BF16),
            vmem((CORES, n_x, block, unit), BF16),
            vmem((n_x, block, CORES * unit), BF16),
            vmem(hops + (n_x * block, unit), BF16),
            vmem(hops + (n_x * block, unit), BF16),
            vmem((n_x * block, unit), F32),
            vmem((tokens, width), F32),
            vmem((tokens, 1), F32),
            vmem((8, tokens), F32),
            vmem((n_t - 1, 8, tokens), F32),
            sems((CORES,)),
            sems((n_x,)),
            sems((n_dp,)),
            sems((n_x, n_t // n_x)),
            sems(hops),
            sems(hops),
            sems((n_x,)),
            sems((n_x,)),
            sems((n_x,)),
            sems((n_x,)),
            sems((CORES, n_x)),
            sems((CORES, n_x)),
            sems(hops),
            sems(hops),
            sems((n_t - 1,)),
            sems((n_t - 1,)),
        ],
        compiler_params=pltpu.CompilerParams(collective_id=2, has_side_effects=True, vmem_limit_bytes=GRANT),
        name="student",
    )(final, dest_row[None, :], hidden, hiddens, w_down, downs, proj, projs, x_all)


def local(
    attn_ctx,
    w_out,
    resid,
    teacher_gain,
    dest_row,
    student_in,
    student_gain,
    w_gate,
    w_up,
    w_down,
    proj,
):
    x_all, gates, ups, downs = gather_rows(student_in, w_gate, w_up, w_down)
    hidden = gated(student_gain, x_all, w_gate, w_up, gates, ups)
    final, hiddens, projs = teacher(attn_ctx, resid, w_out, teacher_gain, hidden, proj)
    out, residue, loss = student(final, dest_row, hidden, hiddens, w_down, downs, proj, projs, x_all)
    return (out, loss[0], residue)


def solution(mesh):
    placed = (
        P("dp", "tensor"),
        P("tensor", None),
        P(("dp", "tensor"), None),
        P(),
        P(),
        P("dp", "tensor"),
        P(),
        P("dp", "tensor"),
        P("dp", "tensor"),
        P("tensor", "dp"),
        P("dp", "tensor"),
    )
    return jax.shard_map(
        local,
        mesh=mesh,
        in_specs=placed,
        out_specs=(P("dp", "tensor"), P("dp"), P("dp", "tensor")),
        check_vma=False,
    )
```

```python
import functools

import jax
import jax.numpy as jnp
from jax import lax
from jax.experimental import pallas as pl
from jax.experimental.pallas import tpu as pltpu
from jax.sharding import PartitionSpec as P

F32 = jnp.float32
BF16 = jnp.bfloat16
CORES = 2
MESH = pl.DeviceIdType.MESH
ANY = pl.BlockSpec(memory_space=pl.ANY)
VMEM = pl.BlockSpec(memory_space=pltpu.VMEM)
GRANT = 62 * 1024 * 1024


class Place:
    def __init__(self):
        self.n_dp = lax.axis_size("dp")
        self.n_t = lax.axis_size("tensor")
        self.n_x = self.n_dp // CORES
        self.n_y = self.n_x if self.n_t % self.n_x == 0 else 1
        self.n_z = self.n_t // self.n_y
        self.far = self.n_t // 2
        self.dp = lax.axis_index("dp")
        self.t = lax.axis_index("tensor")
        self.x = lax.div(self.dp, CORES)
        self.core = lax.rem(self.dp, CORES)
        self.spot = self.spot_of(self.t)
        self.sibling = self.x * CORES + 1 - self.core

    def spot_of(self, t):
        n_y, n_z = self.n_y, self.n_z
        if n_y == 1:
            return t
        z, y = lax.div(t, n_y), lax.rem(t, n_y)
        on = lax.div(y + n_y - 1, n_y)
        r = n_z - 1 - z
        i = y - 1 + lax.rem(r, 2) * (n_y - 2 * y)
        return (1 - on) * z + on * (n_z + r * (n_y - 1) + i)

    def at(self, offset):
        n_y, n_z = self.n_y, self.n_z
        p = lax.rem(self.spot + (offset + self.n_t), self.n_t)
        if n_y == 1:
            return p
        on = lax.div(lax.div(p, n_z) + n_y - 1, n_y)
        q = on * (p - n_z)
        r, i = lax.div(q, n_y - 1), lax.rem(q, n_y - 1)
        z = (1 - on) * p + on * (n_z - 1 - r)
        y = on * (1 + i + lax.rem(r, 2) * (n_y - 2 - 2 * i))
        return z * n_y + y

    def x_at(self, s):
        return lax.rem(self.x + s, self.n_x)

    def peer(self, s):
        return self.x_at(s) * CORES + self.core


def greet(devices):
    barrier = pltpu.get_barrier_semaphore()
    for device in devices:
        pl.semaphore_signal(barrier, inc=1, device_id=device, device_id_type=MESH)
    pl.semaphore_wait(barrier, len(devices))


def push(src, dst, send, recv, device):
    return pltpu.make_async_remote_copy(
        src_ref=src, dst_ref=dst, send_sem=send, recv_sem=recv, device_id=device, device_id_type=MESH
    )


def column_part(w, parts):
    cols = w.shape[1] // parts
    if cols % 128 == 0:
        return w
    return w.reshape(w.shape[0], parts, cols).transpose(1, 0, 2)


def part_of(ref, at, cols):
    if len(ref.shape) == 3:
        return ref.at[at]
    return ref.at[:, pl.ds(pl.multiple_of(at * cols, cols), cols)]


def as_row(column):
    return jnp.transpose(jnp.broadcast_to(column, (column.shape[0], 128)))[:8]


def as_column(row):
    return jnp.transpose(jnp.broadcast_to(row[:1], (128, row.shape[1])))[:, :1]


def add_over(peers, own, got, send, recv):
    copies = [push(own, got.at[k], send.at[k], recv.at[k], peer) for k, peer in enumerate(peers)]
    for copy in copies:
        copy.start()
    total = own[...]
    for k, copy in enumerate(copies):
        copy.wait_recv()
        total = total + got[k]
    for copy in copies:
        copy.wait_send()
    return total


SLOTS = 4


def front_kernel(
    rows_in, s_gain, ctx, resid, t_gain, gate, up, down, w_out, proj,
    out, hiddens, projs, downs, here,
    x_v, g_v, u_v, g_sum, u_sum, squares, hid_v,
    w_v, sums, sent, got, total, row, rows_got,
    own_sem, ring_send, ring_recv, x_send, x_recv, core_send, core_recv,
    hid_send, hid_recv, w_sem, send, recv, row_send, row_recv,
):
    me = Place()
    n_x, n_t, n_dp, far = me.n_x, me.n_t, me.n_dp, me.far
    tokens, d_cols = rows_in.shape
    cols = g_v.shape[2]
    width = w_v.shape[2]
    half = tokens // 2
    own_rows = resid.shape[0]
    line = [(me.dp, me.at(1)), (me.dp, me.at(-1))]
    peers = [(me.peer(s), me.t) for s in range(1, n_x)]
    twin = (me.sibling, me.t)
    plane = [(me.dp, lax.rem(me.t + k, n_t)) for k in range(1, n_t)]

    order = [far]
    for k in range(far - 1, 0, -1):
        order += [k, -k]
    order += [0]
    slot = {k: i % SLOTS for i, k in enumerate(order)}

    def load(k):
        at = pl.ds(pl.multiple_of(me.at(k) * width, width), width)
        return pltpu.make_async_copy(w_out.at[:, at], w_v.at[slot[k]], w_sem.at[slot[k]])

    def reload(k):
        after = order.index(k) + SLOTS
        if after < len(order):
            load(order[after]).start()

    greet(plane + peers + [twin])
    started = []

    def start(copy):
        copy.start()
        started.append(copy)
        return copy

    def ring(k, d, s):
        t = me.at((1 - k) * (1 - 2 * d))
        dst = x_v.at[t, me.x_at(s)]
        src = rows_in if k == 1 and s == 0 else dst
        if k == far:
            at = pl.ds(d * half, half)
            src, dst = src.at[at], dst.at[at]
        at = (d, k - 1, s)
        return push(src, dst, ring_send.at[at], ring_recv.at[at], line[d])

    hops = {}
    for d in range(2):
        hops[1, d, 0] = start(ring(1, d, 0))
    cross = [
        start(push(rows_in, x_v.at[me.t, me.x], x_send.at[0, s], x_recv.at[0, s], peer))
        for s, peer in enumerate(peers)
    ]
    moved = {}
    for i, (w, buf) in enumerate(((gate, g_v), (up, u_v)), 1):
        for s, peer in enumerate(peers):
            moved[i, s] = start(
                push(part_of(w, me.x_at(s + 1), cols), buf.at[me.dp], x_send.at[i, s], x_recv.at[i, s], peer)
            )
    for s, peer in enumerate(peers):
        first = pl.ds(0, proj.shape[0] // 2)
        moved[3, s] = start(
            push(proj.at[first], projs.at[me.dp, first], x_send.at[3, s], x_recv.at[3, s], peer)
        )
    for o in range(min(SLOTS, len(order))):
        load(order[o]).start()
    owns = [
        pltpu.make_async_copy(rows_in, x_v.at[me.t, me.x], own_sem.at[0]),
        pltpu.make_async_copy(part_of(gate, me.x, cols), g_v.at[me.dp], own_sem.at[1]),
        pltpu.make_async_copy(part_of(up, me.x, cols), u_v.at[me.dp], own_sem.at[2]),
    ]
    for copy in owns:
        copy.start()
    early = [
        start(push(part_of(gate, me.x, cols), g_v.at[me.dp], core_send.at[0, 0], core_recv.at[0, 0], twin)),
        start(push(part_of(up, me.x, cols), u_v.at[me.dp], core_send.at[1, 0], core_recv.at[1, 0], twin)),
    ]
    late = [
        start(push(down, downs, core_send.at[2, 0], core_recv.at[2, 0], twin)),
        start(push(proj, projs.at[me.dp], core_send.at[3, 0], core_recv.at[3, 0], twin)),
    ]

    def relay(i, buf, copies):
        for s in range(1, n_x):
            moved[i, s - 1].wait_recv()
            block = buf.at[me.peer(n_x - s)]
            if i == 3:
                block = buf.at[me.peer(n_x - s), pl.ds(0, proj.shape[0] // 2)]
            at = (i if i == 3 else i - 1, s)
            copies.append(start(push(block, block, core_send.at[at], core_recv.at[at], twin)))

    for s in range(1, n_x):
        cross[n_x - s - 1].wait_recv()
        for d in range(2):
            hops[1, d, s] = start(ring(1, d, s))
    for k in range(1, far):
        for s in range(n_x):
            for d in range(2):
                hops[k, d, s].wait_recv()
                hops[k + 1, d, s] = start(ring(k + 1, d, s))
        if k == max(far - 2, 1):
            relay(1, g_v, early)

    tile = min(256, width)

    def term(k, u):
        @pl.loop(0, width // tile)
        def _(c):
            at = pl.ds(pl.multiple_of(c * tile, tile), tile)
            sums[:, at] = jnp.dot(
                ctx[u * half : (u + 1) * half, :], w_v[slot[k], :, at], preferred_element_type=F32
            )

        first = me.t * own_rows

        @pl.when(lax.div(first, half) == u)
        def _():
            rows = pl.ds(pl.multiple_of(first - u * half, own_rows), own_rows)
            at = pl.ds(pl.multiple_of(me.at(k) * width, width), width)
            sums[rows, :] = sums[rows, :] + resid[:, at].astype(F32)

    def hop(k, d, u):
        at = (d, k - 1, u)
        return push(sent.at[at], got.at[at], send.at[at], recv.at[at], line[d])

    load(far).wait()
    for d in range(2):
        term(far, d)
        sent[d, far - 1, d] = sums[...].astype(BF16)
        hop(far, d, d).start()
    reload(far)

    for s in range(n_x):
        for d in range(2):
            hops[far, d, s].wait_recv()
    for copy in owns:
        copy.wait()
    block = here.shape[1]
    per = n_t // n_x
    mine = pl.ds(pl.multiple_of(me.t * block, block), block)
    heres = [
        pltpu.make_async_copy(
            x_v.at[me.x * per + j, x, mine], here.at[x, :, pl.ds(j * d_cols, d_cols)], own_sem.at[3 + x * per + j]
        )
        for x in range(n_x)
        for j in range(per)
    ]
    for copy in heres:
        copy.start()

    strip = min(256, tokens)
    per_dp = n_t // n_dp
    strips = n_x * tokens // strip
    hid = []

    def gated(r):
        x, first = r * strip // tokens, r * strip % tokens

        @pl.loop(0, n_dp)
        def _(i):
            parts = [x_v[i * per_dp + j, x, first : first + strip, :] for j in range(per_dp)]
            rows = jnp.concatenate(parts, axis=1).astype(F32)
            depth = per_dp * d_cols
            weight = s_gain[:, pl.ds(pl.multiple_of(i * depth, depth), depth)].astype(F32)
            scaled = (rows * weight).astype(BF16)
            square = jnp.sum(rows * rows, axis=1, keepdims=True)
            g = jnp.dot(scaled, g_v[i], preferred_element_type=F32)
            u = jnp.dot(scaled, u_v[i], preferred_element_type=F32)

            @pl.when(i == 0)
            def _():
                squares[...] = square
                g_sum[...] = g
                u_sum[...] = u

            @pl.when(i > 0)
            def _():
                squares[...] = squares[...] + square
                g_sum[...] = g_sum[...] + g
                u_sum[...] = u_sum[...] + u

        scale = lax.rsqrt(squares[...] / (n_t * d_cols) + 1e-05)
        g = g_sum[...] * scale
        hid_v[r * strip : (r + 1) * strip, :] = (jax.nn.silu(g) * (u_sum[...] * scale)).astype(BF16)
        at = pl.ds(r * strip, strip)
        copy = pltpu.make_async_copy(hid_v.at[at], hiddens.at[me.x, at], hid_send.at[r, n_x - 1])
        copy.start()
        hid.append(copy)
        for s, peer in enumerate(peers):
            start(push(hid_v.at[at], hiddens.at[me.x, at], hid_send.at[r, s], hid_recv.at[r, s], peer))

    left = list(range(strips))
    turns = [(k, i) for k in range(far - 1, 0, -1) for i in range(2)][1:5]
    for k in range(far - 1, 0, -1):
        for d in range(2):
            load(k if d == 0 else -k).wait()
        for i in range(2):
            for d in range(2):
                u = (d + i + (k == far - 1)) % 2
                term(k if d == 0 else -k, u)
                if k + 1 < far or u == d:
                    hop(k + 1, d, u).wait_recv()
                    sent[d, k - 1, u] = (sums[...] + got[d, k, u].astype(F32)).astype(BF16)
                else:
                    sent[d, k - 1, u] = sums[...].astype(BF16)
                hop(k, d, u).start()
            if k == far - 1 and i == 1:
                relay(2, u_v, early)
                for copy in early:
                    copy.wait_recv()
            if (k, i) in turns:
                for _ in range(-(-strips // len(turns))):
                    if left:
                        gated(left.pop(0))
        reload(k)
        reload(-k)
    while left:
        gated(left.pop(0))
    load(0).wait()
    for i in range(2):
        term(0, i)
        for d in range(2):
            hop(1, d, i).wait_recv()
        total[i * half : (i + 1) * half, :] = (
            sums[...] + got[0, 0, i].astype(F32) + got[1, 0, i].astype(F32)
        )
    row[...] = as_row(jnp.sum(total[...] * total[...], axis=1, keepdims=True))
    relay(3, projs, late)
    sums_of = add_over(plane, row, rows_got, row_send, row_recv)
    scale = as_column(lax.rsqrt(sums_of / (n_t * width) + 1e-06))
    weight = t_gain[:, pl.ds(pl.multiple_of(me.t * width, width), width)].astype(F32)
    out[...] = (total[...] * scale * weight).astype(BF16)
    for copy in late:
        copy.wait_recv()
    for r in range(strips):
        at = pl.ds(r * strip, strip)
        for s, peer in enumerate(peers):
            push(hid_v.at[at], hiddens.at[me.x, at], hid_send.at[r, s], hid_recv.at[r, s], peer).wait_recv()
    for copy in hid + heres:
        copy.wait()
    for copy in started:
        copy.wait_send()
    for d in range(2):
        hop(far, d, d).wait_send()
        for k in range(far - 1, 0, -1):
            for u in range(2):
                hop(k, d, u).wait_send()


def front(student_in, student_gain, attn_ctx, resid, teacher_gain, w_gate, w_up, w_down, w_out, proj):
    n_t, n_dp = lax.axis_size("tensor"), lax.axis_size("dp")
    n_x, far = n_dp // CORES, n_t // 2
    tokens, d_cols = student_in.shape
    ctx_depth = attn_ctx.shape[1]
    width = w_out.shape[1] // n_t
    depth, cols = w_gate.shape[0], w_gate.shape[1] // n_x
    strip = min(256, tokens)
    strips = n_x * tokens // strip
    block, per = tokens // n_t, n_t // n_x
    sems, vmem = pltpu.SemaphoreType.DMA, pltpu.VMEM
    units = (2, far, 2)
    shape = jax.ShapeDtypeStruct
    return pl.pallas_call(
        front_kernel,
        out_shape=(
            shape((tokens, width), BF16),
            shape((n_x, n_x * tokens, cols), BF16),
            shape((n_dp,) + proj.shape, BF16),
            shape(w_down.shape, BF16),
            shape((n_x, block, per * d_cols), BF16),
        ),
        in_specs=[VMEM] * 5 + [ANY] * 5,
        out_specs=(VMEM, ANY, ANY, ANY, ANY),
        scratch_shapes=[
            vmem((n_t, n_x, tokens, d_cols), BF16),
            vmem((n_dp, depth, cols), BF16),
            vmem((n_dp, depth, cols), BF16),
            vmem((strip, cols), F32),
            vmem((strip, cols), F32),
            vmem((strip, 1), F32),
            vmem((n_x * tokens, cols), BF16),
            vmem((SLOTS, ctx_depth, width), BF16),
            vmem((tokens // 2, width), F32),
            vmem(units + (tokens // 2, width), BF16),
            vmem(units + (tokens // 2, width), BF16),
            vmem((tokens, width), F32),
            vmem((8, tokens), F32),
            vmem((n_t - 1, 8, tokens), F32),
            sems((3 + n_x * per,)),
            sems((2, far, n_x)),
            sems((2, far, n_x)),
            sems((4, n_x)),
            sems((4, n_x)),
            sems((4, n_x)),
            sems((4, n_x)),
            sems((strips, n_x)),
            sems((strips, n_x)),
            sems((SLOTS,)),
            sems(units),
            sems(units),
            sems((n_t - 1,)),
            sems((n_t - 1,)),
        ],
        compiler_params=pltpu.CompilerParams(collective_id=0, has_side_effects=True, vmem_limit_bytes=GRANT),
        name="front",
    )(
        student_in, student_gain[None, :], attn_ctx, resid, teacher_gain[None, :],
        column_part(w_gate, n_x), column_part(w_up, n_x), w_down, w_out, proj,
    )


def student_kernel(
    final, dest, here, hiddens, w_down, downs, proj, projs, out, residue, loss,
    d_v, h_v, p_v, fin, full, mixed, sent, got, sums, target, column, row, rows_got,
    d_sem, h_sem, p_sem, send, recv, fin_send, fin_recv, twin_send, twin_recv,
    swap_send, swap_recv, ring_send, ring_recv, row_send, row_recv, rest_send, rest_recv, kin_send, kin_recv,
):
    me = Place()
    n_x, n_t, n_dp, far = me.n_x, me.n_t, me.n_dp, me.far
    cols = h_v.shape[2]
    unit, block = d_v.shape[2], full.shape[3]
    tokens = final.shape[0]
    per = n_t // n_x
    half = sums.shape[1] // 2
    line = [(me.dp, me.at(1)), (me.dp, me.at(-1))]
    peers = [(me.peer(s), me.t) for s in range(1, n_x)]
    twin = (me.sibling, me.t)
    plane = [(me.dp, lax.rem(me.t + k, n_t)) for k in range(1, n_t)]

    def either(mine, index, own, other, dst, sem):
        @pl.when(mine == index)
        def _():
            pltpu.make_async_copy(own, dst, sem).start()

        @pl.when(mine != index)
        def _():
            pltpu.make_async_copy(other, dst, sem).start()

    for x in range(n_x):
        pltpu.make_async_copy(hiddens.at[x], h_v.at[x], h_sem.at[x]).start()
    for u in range(CORES):
        either(me.core, u, w_down, downs, d_v.at[u], d_sem.at[u])
    greet(plane + peers + [twin])
    finals = [
        push(final, fin.at[me.dp], fin_send.at[s], fin_recv.at[s], peer) for s, peer in enumerate(peers)
    ] + [push(final, fin.at[me.dp], twin_send.at[0], twin_recv.at[0], twin)]
    for copy in finals:
        copy.start()
    p_half = proj.shape[0] // 2
    second = pl.ds(p_half, p_half)
    rest_p = [
        push(proj.at[second], p_v.at[me.dp, second], rest_send.at[s], rest_recv.at[s], peer)
        for s, peer in enumerate(peers)
    ]
    for copy in rest_p:
        copy.start()
    fin[me.dp] = final[...]
    column[...] = jnp.zeros_like(column)
    for x in range(n_x):
        pltpu.make_async_copy(hiddens.at[x], h_v.at[x], h_sem.at[x]).wait()

    tile = min(256, unit)

    def term(ks, u):
        spots = [me.at(k) for k in ks]

        @pl.loop(0, unit // tile)
        def _(c):
            at = pl.ds(pl.multiple_of(c * tile, tile), tile)
            total = None
            for x in range(n_x):
                rows = [
                    h_v[x, pl.ds(pl.multiple_of(y * tokens + t * block, block), block), :]
                    for t in spots
                    for y in range(n_x)
                ]
                piece = jnp.dot(
                    jnp.concatenate(rows, axis=0),
                    d_v[u, x * cols : (x + 1) * cols, at],
                    preferred_element_type=F32,
                )
                total = piece if total is None else total + piece
            for i in range(len(ks)):
                sums[i, :, at] = total[i * 2 * half : (i + 1) * 2 * half]

    def hop(k, d, u):
        at = (d, k - 1, u)
        src, dst = sent.at[at], got.at[at]
        if k == far:
            src, dst = src.at[pl.ds(d * half, half)], dst.at[pl.ds(d * half, half)]
        return push(src, dst, send.at[at], recv.at[at], line[d])

    for u in range(CORES):
        pltpu.make_async_copy(w_down, d_v.at[u], d_sem.at[u]).wait()
        term([far], u)
        for d in range(2):
            rows = slice(d * half, (d + 1) * half)
            sent[d, far - 1, u, rows] = sums[0, rows].astype(BF16)
            hop(far, d, u).start()

    def of_proj(i, j, act):
        at = pl.ds(j * p_half, p_half)

        @pl.when(me.dp == i)
        def _():
            act(pltpu.make_async_copy(proj.at[at], p_v.at[i, at], p_sem.at[i, j]))

        @pl.when(me.dp != i)
        def _():
            act(pltpu.make_async_copy(projs.at[i, at], p_v.at[i, at], p_sem.at[i, j]))

    def all_proj(act):
        for i in range(n_dp):
            of_proj(i, 0, act)

            @pl.when(me.x == i // CORES)
            def _():
                of_proj(i, 1, act)

    all_proj(lambda copy: copy.start())
    for k in range(far - 1, 0, -1):
        for u in range(CORES):
            term([k, -k], u)
            for d in range(2):
                hop(k + 1, d, u).wait_recv()
                if k + 1 == far:
                    rows, rest = (slice(d * half, (d + 1) * half), slice((1 - d) * half, (2 - d) * half))
                    sent[d, k - 1, u, rows] = (sums[d, rows] + got[d, k, u, rows].astype(F32)).astype(BF16)
                    sent[d, k - 1, u, rest] = sums[d, rest].astype(BF16)
                else:
                    sent[d, k - 1, u] = (sums[d] + got[d, k, u].astype(F32)).astype(BF16)
                hop(k, d, u).start()
    swaps = []
    for u in range(CORES):
        term([0], u)
        for d in range(2):
            hop(1, d, u).wait_recv()
        mlp = sums[0] + got[0, 0, u].astype(F32) + got[1, 0, u].astype(F32)
        known = here[:, :, u * unit : (u + 1) * unit].astype(F32)
        mixed[u] = (known + mlp.reshape(n_x, block, unit)).astype(BF16)
        full[me.t, u, me.x] = mixed[u, me.x]
        for s, peer in enumerate(peers):
            at = (u, s)
            copy = push(mixed.at[u, me.x_at(s + 1)], full.at[me.t, u, me.x], swap_send.at[at], swap_recv.at[at], peer)
            copy.start()
            swaps.append(copy)

    for s in range(1, n_x):
        finals[s - 1].wait_recv()
        piece = fin.at[me.peer(n_x - s)]
        copy = push(piece, piece, twin_send.at[s], twin_recv.at[s], twin)
        copy.start()
        finals.append(copy)
    kin = []
    for s in range(1, n_x):
        rest_p[s - 1].wait_recv()
        piece = p_v.at[me.peer(n_x - s), second]
        copy = push(piece, piece, kin_send.at[s], kin_recv.at[s], twin)
        copy.start()
        kin.append(copy)

    def ring(k, d, u):
        t = me.at((1 - k) * (1 - 2 * d))
        view = full.at[t, u]
        if k == far:
            view = full.at[t, u, :, pl.ds(d * (block // 2), block // 2)]
        at = (d, k - 1, u)
        return push(view, view, ring_send.at[at], ring_recv.at[at], line[d])

    for u in range(CORES):
        for s in range(n_x - 1):
            swaps[u * (n_x - 1) + s].wait_recv()
        for d in range(2):
            ring(1, d, u).start()

    for copy in finals[n_x - 1 :]:
        copy.wait_recv()
    strip = min(256, tokens)

    @pl.loop(0, tokens // strip)
    def _(r):
        first = pl.multiple_of(r * strip, strip)
        places = me.dp * tokens + first + lax.broadcasted_iota(jnp.int32, (strip, tokens), 0)
        total = None
        for i in range(n_dp):
            pick = (places == dest[:, i * tokens : (i + 1) * tokens]).astype(F32).astype(BF16)
            piece = jnp.dot(pick, fin[i], preferred_element_type=F32)
            total = piece if total is None else total + piece
        target[pl.ds(first, strip), :] = total

    all_proj(lambda copy: copy.wait())
    for copy in kin:
        copy.wait_recv()
    p_tile = min(256, target.shape[1])

    def project(ts):
        @pl.loop(0, target.shape[1] // p_tile)
        def _(c):
            at = pl.ds(pl.multiple_of(c * p_tile, p_tile), p_tile)
            total = None
            for x in range(n_x):
                for u in range(CORES):
                    rows = jnp.concatenate([full[t, u, x] for t in ts], axis=0)
                    piece = jnp.dot(rows, p_v[x * CORES + u, :, at], preferred_element_type=F32)
                    total = piece if total is None else total + piece
            for i, t in enumerate(ts):
                rows = pl.ds(pl.multiple_of(t * block, block), block)
                gap = total[i * block : (i + 1) * block] - target[rows, at]
                residue[rows, at] = gap
                column[rows, :] = column[rows, :] + jnp.sum(gap * gap, axis=1, keepdims=True)

    project([me.t])
    for k in range(1, far + 1):
        for u in range(CORES):
            for d in range(2):
                ring(k, d, u).wait_recv()
                if k < far:
                    ring(k + 1, d, u).start()
        project([me.at(-k), me.at(k)] if k < far else [me.at(far)])

    row[...] = as_row(column[...])
    out_cols = out.shape[1]
    x = lax.div(me.t, per)
    u = lax.div(lax.rem(me.t, per) * out_cols, unit)
    inner = pl.multiple_of(lax.rem(me.t * out_cols, unit), out_cols)
    for t in range(n_t):
        out[t * block : (t + 1) * block, :] = full[t, u, x, :, pl.ds(inner, out_cols)]
    loss[...] = add_over(plane, row, rows_got, row_send, row_recv) / (n_t * target.shape[1])
    for u in range(CORES):
        for d in range(2):
            for k in range(1, far + 1):
                hop(k, d, u).wait_send()
                ring(k, d, u).wait_send()
    for copy in finals + swaps + rest_p + kin:
        copy.wait_send()


def student(final, dest_row, here, hiddens, w_down, downs, proj, projs):
    n_t, n_dp = lax.axis_size("tensor"), lax.axis_size("dp")
    n_x, far = n_dp // CORES, n_t // 2
    tokens, width = final.shape
    ff, unit = w_down.shape
    rows, cols = hiddens.shape[1:]
    block = tokens // n_t
    d_cols = CORES * unit * n_x // n_t
    sems = pltpu.SemaphoreType.DMA
    hops = (2, far, CORES)
    vmem = pltpu.VMEM
    return pl.pallas_call(
        student_kernel,
        out_shape=(
            jax.ShapeDtypeStruct((tokens, d_cols), BF16),
            jax.ShapeDtypeStruct((tokens, width), F32),
            jax.ShapeDtypeStruct((8, tokens), F32),
        ),
        in_specs=[VMEM] * 3 + [ANY] * 5,
        out_specs=(VMEM, VMEM, VMEM),
        scratch_shapes=[
            vmem((CORES, ff, unit), BF16),
            vmem((n_x, rows, cols), BF16),
            vmem((n_dp,) + proj.shape, BF16),
            vmem((n_dp, tokens, width), BF16),
            vmem((n_t, CORES, n_x, block, unit), BF16),
            vmem((CORES, n_x, block, unit), BF16),
            vmem(hops + (n_x * block, unit), BF16),
            vmem(hops + (n_x * block, unit), BF16),
            vmem((2, n_x * block, unit), F32),
            vmem((tokens, width), F32),
            vmem((tokens, 1), F32),
            vmem((8, tokens), F32),
            vmem((n_t - 1, 8, tokens), F32),
            sems((CORES,)),
            sems((n_x,)),
            sems((n_dp, 2)),
            sems(hops),
            sems(hops),
            sems((n_x,)),
            sems((n_x,)),
            sems((n_x,)),
            sems((n_x,)),
            sems((CORES, n_x)),
            sems((CORES, n_x)),
            sems(hops),
            sems(hops),
            sems((n_t - 1,)),
            sems((n_t - 1,)),
            sems((n_x,)),
            sems((n_x,)),
            sems((n_x,)),
            sems((n_x,)),
        ],
        compiler_params=pltpu.CompilerParams(collective_id=2, has_side_effects=True, vmem_limit_bytes=GRANT),
        name="student",
    )(final, dest_row[None, :], here, hiddens, w_down, downs, proj, projs)


def local(
    attn_ctx,
    w_out,
    resid,
    teacher_gain,
    dest_row,
    student_in,
    student_gain,
    w_gate,
    w_up,
    w_down,
    proj,
):
    final, hiddens, projs, downs, here = front(
        student_in, student_gain, attn_ctx, resid, teacher_gain, w_gate, w_up, w_down, w_out, proj
    )
    out, residue, loss = student(final, dest_row, here, hiddens, w_down, downs, proj, projs)
    return (out, loss[0], residue)


def solution(mesh):
    placed = (
        P("dp", "tensor"),
        P("tensor", None),
        P(("dp", "tensor"), None),
        P(),
        P(),
        P("dp", "tensor"),
        P(),
        P("dp", "tensor"),
        P("dp", "tensor"),
        P("tensor", "dp"),
        P("dp", "tensor"),
    )
    return jax.shard_map(
        local,
        mesh=mesh,
        in_specs=placed,
        out_specs=(P("dp", "tensor"), P("dp"), P("dp", "tensor")),
        check_vma=False,
    )
```

```python
import functools

import jax
import jax.numpy as jnp
from jax import lax
from jax.experimental import pallas as pl
from jax.experimental.pallas import tpu as pltpu
from jax.sharding import PartitionSpec as P

F32 = jnp.float32
BF16 = jnp.bfloat16
CORES = 2
MESH = pl.DeviceIdType.MESH
ANY = pl.BlockSpec(memory_space=pl.ANY)
VMEM = pl.BlockSpec(memory_space=pltpu.VMEM)
GRANT = 62 * 1024 * 1024


class Place:
    def __init__(self):
        self.n_dp = lax.axis_size("dp")
        self.n_t = lax.axis_size("tensor")
        self.n_x = self.n_dp // CORES
        self.n_y = self.n_x if self.n_t % self.n_x == 0 else 1
        self.n_z = self.n_t // self.n_y
        self.far = self.n_t // 2
        self.dp = lax.axis_index("dp")
        self.t = lax.axis_index("tensor")
        self.x = lax.div(self.dp, CORES)
        self.core = lax.rem(self.dp, CORES)
        self.spot = self.spot_of(self.t)
        self.sibling = self.x * CORES + 1 - self.core

    def spot_of(self, t):
        n_y, n_z = self.n_y, self.n_z
        if n_y == 1:
            return t
        z, y = lax.div(t, n_y), lax.rem(t, n_y)
        on = lax.div(y + n_y - 1, n_y)
        r = n_z - 1 - z
        i = y - 1 + lax.rem(r, 2) * (n_y - 2 * y)
        return (1 - on) * z + on * (n_z + r * (n_y - 1) + i)

    def at(self, offset):
        n_y, n_z = self.n_y, self.n_z
        p = lax.rem(self.spot + (offset + self.n_t), self.n_t)
        if n_y == 1:
            return p
        on = lax.div(lax.div(p, n_z) + n_y - 1, n_y)
        q = on * (p - n_z)
        r, i = lax.div(q, n_y - 1), lax.rem(q, n_y - 1)
        z = (1 - on) * p + on * (n_z - 1 - r)
        y = on * (1 + i + lax.rem(r, 2) * (n_y - 2 - 2 * i))
        return z * n_y + y

    def x_at(self, s):
        return lax.rem(self.x + s, self.n_x)

    def peer(self, s):
        return self.x_at(s) * CORES + self.core


def greet(devices):
    barrier = pltpu.get_barrier_semaphore()
    for device in devices:
        pl.semaphore_signal(barrier, inc=1, device_id=device, device_id_type=MESH)
    pl.semaphore_wait(barrier, len(devices))


def push(src, dst, send, recv, device):
    return pltpu.make_async_remote_copy(
        src_ref=src, dst_ref=dst, send_sem=send, recv_sem=recv, device_id=device, device_id_type=MESH
    )


def column_part(w, parts):
    cols = w.shape[1] // parts
    if cols % 128 == 0:
        return w
    return w.reshape(w.shape[0], parts, cols).transpose(1, 0, 2)


def part_of(ref, at, cols):
    if len(ref.shape) == 3:
        return ref.at[at]
    return ref.at[:, pl.ds(pl.multiple_of(at * cols, cols), cols)]


def as_row(column):
    return jnp.transpose(jnp.broadcast_to(column, (column.shape[0], 128)))[:8]


def as_column(row):
    return jnp.transpose(jnp.broadcast_to(row[:1], (128, row.shape[1])))[:, :1]


def spread(peers, own, got, send, recv):
    copies = [push(own, got.at[k], send.at[k], recv.at[k], peer) for k, peer in enumerate(peers)]
    for copy in copies:
        copy.start()
    return copies


def add_up(copies, own, got):
    total = own[...]
    for k, copy in enumerate(copies):
        copy.wait_recv()
        total = total + got[k]
    for copy in copies:
        copy.wait_send()
    return total


SLOTS = 4


def front_kernel(
    rows_in, s_gain, ctx, resid, gate, up, down, w_out, proj,
    out, hiddens, projs, downs, here,
    x_v, g_v, u_v, g_sum, u_sum, squares, hid_v,
    w_v, sums, sent, got, total,
    own_sem, out_sem, ring_send, ring_recv, x_send, x_recv, core_send, core_recv,
    hid_send, hid_recv, w_sem, send, recv,
):
    me = Place()
    n_x, n_t, n_dp, far = me.n_x, me.n_t, me.n_dp, me.far
    tokens, d_cols = rows_in.shape
    cols = g_v.shape[2]
    width = w_v.shape[2]
    half = tokens // 2
    own_rows = resid.shape[0]
    line = [(me.dp, me.at(1)), (me.dp, me.at(-1))]
    peers = [(me.peer(s), me.t) for s in range(1, n_x)]
    twin = (me.sibling, me.t)

    order = [far]
    for k in range(far - 1, 0, -1):
        order += [k, -k]
    order += [0]
    slot = {k: i % SLOTS for i, k in enumerate(order)}

    def load(k):
        at = pl.ds(pl.multiple_of(me.at(k) * width, width), width)
        return pltpu.make_async_copy(w_out.at[:, at], w_v.at[slot[k]], w_sem.at[slot[k]])

    def reload(k):
        after = order.index(k) + SLOTS
        if after < len(order):
            load(order[after]).start()

    greet(line + peers + [twin])
    started = []

    def start(copy):
        copy.start()
        started.append(copy)
        return copy

    def ring(k, d, s):
        t = me.at((1 - k) * (1 - 2 * d))
        dst = x_v.at[t, me.x_at(s)]
        src = rows_in if k == 1 and s == 0 else dst
        if k == far:
            at = pl.ds(d * half, half)
            src, dst = src.at[at], dst.at[at]
        at = (d, k - 1, s)
        return push(src, dst, ring_send.at[at], ring_recv.at[at], line[d])

    hops = {}
    for d in range(2):
        hops[1, d, 0] = start(ring(1, d, 0))
    cross = [
        start(push(rows_in, x_v.at[me.t, me.x], x_send.at[0, s], x_recv.at[0, s], peer))
        for s, peer in enumerate(peers)
    ]
    moved = {}
    for i, (w, buf) in enumerate(((gate, g_v), (up, u_v)), 1):
        for s, peer in enumerate(peers):
            moved[i, s] = start(
                push(part_of(w, me.x_at(s + 1), cols), buf.at[me.dp], x_send.at[i, s], x_recv.at[i, s], peer)
            )
    for s, peer in enumerate(peers):
        first = pl.ds(0, proj.shape[0] * 3 // 4)
        moved[3, s] = start(
            push(proj.at[first], projs.at[me.dp, first], x_send.at[3, s], x_recv.at[3, s], peer)
        )
    for o in range(min(SLOTS, len(order))):
        load(order[o]).start()
    owns = [
        pltpu.make_async_copy(rows_in, x_v.at[me.t, me.x], own_sem.at[0]),
        pltpu.make_async_copy(part_of(gate, me.x, cols), g_v.at[me.dp], own_sem.at[1]),
        pltpu.make_async_copy(part_of(up, me.x, cols), u_v.at[me.dp], own_sem.at[2]),
    ]
    for copy in owns:
        copy.start()
    early = [
        start(push(part_of(gate, me.x, cols), g_v.at[me.dp], core_send.at[0, 0], core_recv.at[0, 0], twin)),
        start(push(part_of(up, me.x, cols), u_v.at[me.dp], core_send.at[1, 0], core_recv.at[1, 0], twin)),
    ]
    late = [
        start(push(down, downs, core_send.at[2, 0], core_recv.at[2, 0], twin)),
        start(push(proj, projs.at[me.dp], core_send.at[3, 0], core_recv.at[3, 0], twin)),
    ]

    def relay(i, buf, copies):
        for s in range(1, n_x):
            moved[i, s - 1].wait_recv()
            block = buf.at[me.peer(n_x - s)]
            if i == 3:
                block = buf.at[me.peer(n_x - s), pl.ds(0, proj.shape[0] * 3 // 4)]
            at = (i if i == 3 else i - 1, s)
            copies.append(start(push(block, block, core_send.at[at], core_recv.at[at], twin)))

    for s in range(1, n_x):
        cross[n_x - s - 1].wait_recv()
        for d in range(2):
            hops[1, d, s] = start(ring(1, d, s))
    for k in range(1, far):
        for s in range(n_x):
            for d in range(2):
                hops[k, d, s].wait_recv()
                hops[k + 1, d, s] = start(ring(k + 1, d, s))
        if k == max(far - 2, 1):
            relay(1, g_v, early)

    tile = min(256, width)

    def term(k, u):
        @pl.loop(0, width // tile)
        def _(c):
            at = pl.ds(pl.multiple_of(c * tile, tile), tile)
            sums[:, at] = jnp.dot(
                ctx[u * half : (u + 1) * half, :], w_v[slot[k], :, at], preferred_element_type=F32
            )

        first = me.t * own_rows

        @pl.when(lax.div(first, half) == u)
        def _():
            rows = pl.ds(pl.multiple_of(first - u * half, own_rows), own_rows)
            at = pl.ds(pl.multiple_of(me.at(k) * width, width), width)
            sums[rows, :] = sums[rows, :] + resid[:, at].astype(F32)

    def hop(k, d, u):
        at = (d, k - 1, u)
        return push(sent.at[at], got.at[at], send.at[at], recv.at[at], line[d])

    load(far).wait()
    for d in range(2):
        term(far, d)
        sent[d, far - 1, d] = sums[...].astype(BF16)
        hop(far, d, d).start()
    reload(far)

    for s in range(n_x):
        for d in range(2):
            hops[far, d, s].wait_recv()
    for copy in owns:
        copy.wait()
    block = here.shape[1]
    per = n_t // n_x
    mine = pl.ds(pl.multiple_of(me.t * block, block), block)
    heres = [
        pltpu.make_async_copy(
            x_v.at[me.x * per + j, x, mine], here.at[x, :, pl.ds(j * d_cols, d_cols)], own_sem.at[3 + x * per + j]
        )
        for x in range(n_x)
        for j in range(per)
    ]
    for copy in heres:
        copy.start()

    strip = min(256, tokens)
    per_dp = n_t // n_dp
    strips = n_x * tokens // strip
    hid = []

    def gated(r):
        x, first = r * strip // tokens, r * strip % tokens

        @pl.loop(0, n_dp)
        def _(i):
            parts = [x_v[i * per_dp + j, x, first : first + strip, :] for j in range(per_dp)]
            rows = jnp.concatenate(parts, axis=1).astype(F32)
            depth = per_dp * d_cols
            weight = s_gain[:, pl.ds(pl.multiple_of(i * depth, depth), depth)].astype(F32)
            scaled = (rows * weight).astype(BF16)
            square = jnp.sum(rows * rows, axis=1, keepdims=True)
            g = jnp.dot(scaled, g_v[i], preferred_element_type=F32)
            u = jnp.dot(scaled, u_v[i], preferred_element_type=F32)

            @pl.when(i == 0)
            def _():
                squares[...] = square
                g_sum[...] = g
                u_sum[...] = u

            @pl.when(i > 0)
            def _():
                squares[...] = squares[...] + square
                g_sum[...] = g_sum[...] + g
                u_sum[...] = u_sum[...] + u

        scale = lax.rsqrt(squares[...] / (n_t * d_cols) + 1e-05)
        g = g_sum[...] * scale
        hid_v[r * strip : (r + 1) * strip, :] = (jax.nn.silu(g) * (u_sum[...] * scale)).astype(BF16)
        at = pl.ds(r * strip, strip)
        copy = pltpu.make_async_copy(hid_v.at[at], hiddens.at[me.x, at], hid_send.at[r, n_x - 1])
        copy.start()
        hid.append(copy)
        for s, peer in enumerate(peers):
            start(push(hid_v.at[at], hiddens.at[me.x, at], hid_send.at[r, s], hid_recv.at[r, s], peer))

    left = list(range(strips))
    turns = [(k, i) for k in range(far - 1, 0, -1) for i in range(2)][1:5]
    for k in range(far - 1, 0, -1):
        for d in range(2):
            load(k if d == 0 else -k).wait()
        for i in range(2):
            for d in range(2):
                u = (d + i + (k == far - 1)) % 2
                term(k if d == 0 else -k, u)
                if k + 1 < far or u == d:
                    hop(k + 1, d, u).wait_recv()
                    sent[d, k - 1, u] = (sums[...] + got[d, k, u].astype(F32)).astype(BF16)
                else:
                    sent[d, k - 1, u] = sums[...].astype(BF16)
                hop(k, d, u).start()
            if k == far - 1 and i == 1:
                relay(2, u_v, early)
                for copy in early:
                    copy.wait_recv()
            if (k, i) in turns:
                for _ in range(-(-strips // len(turns))):
                    if left:
                        gated(left.pop(0))
        reload(k)
        reload(-k)
    while left:
        gated(left.pop(0))
    load(0).wait()
    for i in range(2):
        term(0, i)
        for d in range(2):
            hop(1, d, i).wait_recv()
        at = pl.ds(i * half, half)
        total[at, :] = sums[...] + got[0, 0, i].astype(F32) + got[1, 0, i].astype(F32)
        copy = pltpu.make_async_copy(total.at[at], out.at[at], out_sem.at[i])
        copy.start()
        hid.append(copy)
        if i == 0:
            relay(3, projs, late)
    for copy in late:
        copy.wait_recv()
    for r in range(strips):
        at = pl.ds(r * strip, strip)
        for s, peer in enumerate(peers):
            push(hid_v.at[at], hiddens.at[me.x, at], hid_send.at[r, s], hid_recv.at[r, s], peer).wait_recv()
    for copy in hid + heres:
        copy.wait()
    for copy in started:
        copy.wait_send()
    for d in range(2):
        hop(far, d, d).wait_send()
        for k in range(far - 1, 0, -1):
            for u in range(2):
                hop(k, d, u).wait_send()


def front(student_in, student_gain, attn_ctx, resid, w_gate, w_up, w_down, w_out, proj):
    n_t, n_dp = lax.axis_size("tensor"), lax.axis_size("dp")
    n_x, far = n_dp // CORES, n_t // 2
    tokens, d_cols = student_in.shape
    ctx_depth = attn_ctx.shape[1]
    width = w_out.shape[1] // n_t
    depth, cols = w_gate.shape[0], w_gate.shape[1] // n_x
    strip = min(256, tokens)
    strips = n_x * tokens // strip
    block, per = tokens // n_t, n_t // n_x
    sems, vmem = pltpu.SemaphoreType.DMA, pltpu.VMEM
    units = (2, far, 2)
    shape = jax.ShapeDtypeStruct
    return pl.pallas_call(
        front_kernel,
        out_shape=(
            shape((tokens, width), F32),
            shape((n_x, n_x * tokens, cols), BF16),
            shape((n_dp,) + proj.shape, BF16),
            shape(w_down.shape, BF16),
            shape((n_x, block, per * d_cols), BF16),
        ),
        in_specs=[VMEM] * 4 + [ANY] * 5,
        out_specs=(ANY,) * 5,
        scratch_shapes=[
            vmem((n_t, n_x, tokens, d_cols), BF16),
            vmem((n_dp, depth, cols), BF16),
            vmem((n_dp, depth, cols), BF16),
            vmem((strip, cols), F32),
            vmem((strip, cols), F32),
            vmem((strip, 1), F32),
            vmem((n_x * tokens, cols), BF16),
            vmem((SLOTS, ctx_depth, width), BF16),
            vmem((tokens // 2, width), F32),
            vmem(units + (tokens // 2, width), BF16),
            vmem(units + (tokens // 2, width), BF16),
            vmem((tokens, width), F32),
            sems((3 + n_x * per,)),
            sems((2,)),
            sems((2, far, n_x)),
            sems((2, far, n_x)),
            sems((4, n_x)),
            sems((4, n_x)),
            sems((4, n_x)),
            sems((4, n_x)),
            sems((strips, n_x)),
            sems((strips, n_x)),
            sems((SLOTS,)),
            sems(units),
            sems(units),
        ],
        compiler_params=pltpu.CompilerParams(collective_id=0, has_side_effects=True, vmem_limit_bytes=GRANT),
        name="front",
    )(
        student_in, student_gain[None, :], attn_ctx, resid,
        column_part(w_gate, n_x), column_part(w_up, n_x), w_down, w_out, proj,
    )


def student_kernel(
    t_gain, dest, here, raw, hiddens, w_down, downs, proj, projs, out, residue, loss,
    raw_v, final, squares, squares_got, d_v, h_v, p_v, fin, full, mixed, sent, got, sums, target, column, row, rows_got,
    d_sem, h_sem, p_sem, send, recv, fin_send, fin_recv, twin_send, twin_recv,
    swap_send, swap_recv, ring_send, ring_recv, row_send, row_recv, rest_send, rest_recv, kin_send, kin_recv,
    raw_sem, square_send, square_recv,
):
    me = Place()
    n_x, n_t, n_dp, far = me.n_x, me.n_t, me.n_dp, me.far
    cols = h_v.shape[2]
    unit, block = d_v.shape[2], full.shape[3]
    tokens = final.shape[0]
    per = n_t // n_x
    half = sums.shape[1] // 2
    line = [(me.dp, me.at(1)), (me.dp, me.at(-1))]
    peers = [(me.peer(s), me.t) for s in range(1, n_x)]
    twin = (me.sibling, me.t)
    plane = [(me.dp, lax.rem(me.t + k, n_t)) for k in range(1, n_t)]

    def either(mine, index, own, other, dst, sem):
        @pl.when(mine == index)
        def _():
            pltpu.make_async_copy(own, dst, sem).start()

        @pl.when(mine != index)
        def _():
            pltpu.make_async_copy(other, dst, sem).start()

    raw_copy = pltpu.make_async_copy(raw, raw_v, raw_sem)
    raw_copy.start()
    for x in range(n_x):
        pltpu.make_async_copy(hiddens.at[x], h_v.at[x], h_sem.at[x]).start()
    either(me.core, 0, w_down, downs, d_v.at[0], d_sem.at[0])
    greet(plane + peers + [twin])
    p_first = proj.shape[0] * 3 // 4
    second = pl.ds(p_first, proj.shape[0] - p_first)
    rest_p = [
        push(proj.at[second], p_v.at[me.dp, second], rest_send.at[s], rest_recv.at[s], peer)
        for s, peer in enumerate(peers)
    ]
    for copy in rest_p:
        copy.start()
    raw_copy.wait()
    squares[...] = as_row(jnp.sum(raw_v[...] * raw_v[...], axis=1, keepdims=True))
    shared = spread(plane, squares, squares_got, square_send, square_recv)
    for x in range(n_x):
        pltpu.make_async_copy(hiddens.at[x], h_v.at[x], h_sem.at[x]).wait()
    for u in range(1, CORES):
        either(me.core, u, w_down, downs, d_v.at[u], d_sem.at[u])
    column[...] = jnp.zeros_like(column)

    tile = min(256, unit)

    def term(ks, u):
        spots = [me.at(k) for k in ks]

        @pl.loop(0, unit // tile)
        def _(c):
            at = pl.ds(pl.multiple_of(c * tile, tile), tile)
            total = None
            for x in range(n_x):
                rows = [
                    h_v[x, pl.ds(pl.multiple_of(y * tokens + t * block, block), block), :]
                    for t in spots
                    for y in range(n_x)
                ]
                piece = jnp.dot(
                    jnp.concatenate(rows, axis=0),
                    d_v[u, x * cols : (x + 1) * cols, at],
                    preferred_element_type=F32,
                )
                total = piece if total is None else total + piece
            for i in range(len(ks)):
                sums[i, :, at] = total[i * 2 * half : (i + 1) * 2 * half]

    def hop(k, d, u):
        at = (d, k - 1, u)
        src, dst = sent.at[at], got.at[at]
        if k == far:
            src, dst = src.at[pl.ds(d * half, half)], dst.at[pl.ds(d * half, half)]
        return push(src, dst, send.at[at], recv.at[at], line[d])

    def of_proj(i, j, act):
        at = second if j else pl.ds(0, p_first)

        @pl.when(me.dp == i)
        def _():
            act(pltpu.make_async_copy(proj.at[at], p_v.at[i, at], p_sem.at[i, j]))

        @pl.when(me.dp != i)
        def _():
            act(pltpu.make_async_copy(projs.at[i, at], p_v.at[i, at], p_sem.at[i, j]))

    def all_proj(act):
        for i in range(n_dp):
            of_proj(i, 0, act)

            @pl.when(me.x == i // CORES)
            def _():
                of_proj(i, 1, act)

    swaps = {}

    def first_hop(u):
        pltpu.make_async_copy(w_down, d_v.at[u], d_sem.at[u]).wait()
        term([far], u)
        for d in range(2):
            rows = slice(d * half, (d + 1) * half)
            sent[d, far - 1, u, rows] = sums[0, rows].astype(BF16)
            hop(far, d, u).start()

    def next_hop(k, u):
        term([k, -k], u)
        for d in range(2):
            hop(k + 1, d, u).wait_recv()
            if k + 1 == far:
                rows, rest = (slice(d * half, (d + 1) * half), slice((1 - d) * half, (2 - d) * half))
                sent[d, k - 1, u, rows] = (sums[d, rows] + got[d, k, u, rows].astype(F32)).astype(BF16)
                sent[d, k - 1, u, rest] = sums[d, rest].astype(BF16)
            else:
                sent[d, k - 1, u] = (sums[d] + got[d, k, u].astype(F32)).astype(BF16)
            hop(k, d, u).start()

    def last_hop(u):
        term([0], u)
        for d in range(2):
            hop(1, d, u).wait_recv()
        mlp = sums[0] + got[0, 0, u].astype(F32) + got[1, 0, u].astype(F32)
        known = here[:, :, u * unit : (u + 1) * unit].astype(F32)
        mixed[u] = (known + mlp.reshape(n_x, block, unit)).astype(BF16)
        full[me.t, u, me.x] = mixed[u, me.x]
        for s, peer in enumerate(peers):
            at = (u, s)
            swaps[at] = push(
                mixed.at[u, me.x_at(s + 1)], full.at[me.t, u, me.x], swap_send.at[at], swap_recv.at[at], peer
            )
            swaps[at].start()

    def ring(k, d, u):
        t = me.at((1 - k) * (1 - 2 * d))
        view = full.at[t, u]
        if k == far:
            view = full.at[t, u, :, pl.ds(d * (block // 2), block // 2)]
        at = (d, k - 1, u)
        return push(view, view, ring_send.at[at], ring_recv.at[at], line[d])

    def gather(u):
        for s in range(n_x - 1):
            swaps[u, s].wait_recv()
        for d in range(2):
            ring(1, d, u).start()

    finals = []
    for stage in range(far + 2):
        for u in range(CORES):
            k = far - stage + u
            if k == far:
                first_hop(u)
            elif 0 < k < far:
                next_hop(k, u)
            elif k == 0:
                last_hop(u)
            if stage == 1 and u == 0:
                all_proj(lambda copy: copy.start())
            if stage == far and u == 1:
                gather(0)
        if stage == 1:
            scale = as_column(lax.rsqrt(add_up(shared, squares, squares_got) / (n_t * target.shape[1]) + 1e-06))
            width = target.shape[1]
            weight = t_gain[:, pl.ds(pl.multiple_of(me.t * width, width), width)].astype(F32)
            final[...] = (raw_v[...] * scale * weight).astype(BF16)
            fin[me.dp] = final[...]
            finals += [
                push(final, fin.at[me.dp], fin_send.at[s], fin_recv.at[s], peer) for s, peer in enumerate(peers)
            ] + [push(final, fin.at[me.dp], twin_send.at[0], twin_recv.at[0], twin)]
            for copy in finals:
                copy.start()
    gather(1)

    for s in range(1, n_x):
        finals[s - 1].wait_recv()
        piece = fin.at[me.peer(n_x - s)]
        copy = push(piece, piece, twin_send.at[s], twin_recv.at[s], twin)
        copy.start()
        finals.append(copy)
    kin = []
    for s in range(1, n_x):
        rest_p[s - 1].wait_recv()
        piece = p_v.at[me.peer(n_x - s), second]
        copy = push(piece, piece, kin_send.at[s], kin_recv.at[s], twin)
        copy.start()
        kin.append(copy)

    for copy in finals[n_x - 1 :]:
        copy.wait_recv()
    strip = min(256, tokens)

    @pl.loop(0, tokens // strip)
    def _(r):
        first = pl.multiple_of(r * strip, strip)
        places = me.dp * tokens + first + lax.broadcasted_iota(jnp.int32, (strip, tokens), 0)
        total = None
        for i in range(n_dp):
            pick = (places == dest[:, i * tokens : (i + 1) * tokens]).astype(F32).astype(BF16)
            piece = jnp.dot(pick, fin[i], preferred_element_type=F32)
            total = piece if total is None else total + piece
        target[pl.ds(first, strip), :] = total

    all_proj(lambda copy: copy.wait())
    for copy in kin:
        copy.wait_recv()
    p_tile = min(256, target.shape[1])

    def project(ts):
        @pl.loop(0, target.shape[1] // p_tile)
        def _(c):
            at = pl.ds(pl.multiple_of(c * p_tile, p_tile), p_tile)
            total = None
            for x in range(n_x):
                for u in range(CORES):
                    rows = jnp.concatenate([full[t, u, x] for t in ts], axis=0)
                    piece = jnp.dot(rows, p_v[x * CORES + u, :, at], preferred_element_type=F32)
                    total = piece if total is None else total + piece
            for i, t in enumerate(ts):
                rows = pl.ds(pl.multiple_of(t * block, block), block)
                gap = total[i * block : (i + 1) * block] - target[rows, at]
                residue[rows, at] = gap
                column[rows, :] = column[rows, :] + jnp.sum(gap * gap, axis=1, keepdims=True)

    project([me.t])
    for k in range(1, far + 1):
        for u in range(CORES):
            for d in range(2):
                ring(k, d, u).wait_recv()
                if k < far:
                    ring(k + 1, d, u).start()
        project([me.at(-k), me.at(k)] if k < far else [me.at(far)])

    row[...] = as_row(column[...])
    out_cols = out.shape[1]
    x = lax.div(me.t, per)
    u = lax.div(lax.rem(me.t, per) * out_cols, unit)
    inner = pl.multiple_of(lax.rem(me.t * out_cols, unit), out_cols)
    for t in range(n_t):
        out[t * block : (t + 1) * block, :] = full[t, u, x, :, pl.ds(inner, out_cols)]
    loss[...] = add_up(spread(plane, row, rows_got, row_send, row_recv), row, rows_got) / (n_t * target.shape[1])
    for u in range(CORES):
        for d in range(2):
            for k in range(1, far + 1):
                hop(k, d, u).wait_send()
                ring(k, d, u).wait_send()
    for copy in finals + list(swaps.values()) + rest_p + kin:
        copy.wait_send()


def student(raw, teacher_gain, dest_row, here, hiddens, w_down, downs, proj, projs):
    n_t, n_dp = lax.axis_size("tensor"), lax.axis_size("dp")
    n_x, far = n_dp // CORES, n_t // 2
    tokens, width = raw.shape
    ff, unit = w_down.shape
    rows, cols = hiddens.shape[1:]
    block = tokens // n_t
    d_cols = CORES * unit * n_x // n_t
    sems = pltpu.SemaphoreType.DMA
    hops = (2, far, CORES)
    vmem = pltpu.VMEM
    return pl.pallas_call(
        student_kernel,
        out_shape=(
            jax.ShapeDtypeStruct((tokens, d_cols), BF16),
            jax.ShapeDtypeStruct((tokens, width), F32),
            jax.ShapeDtypeStruct((8, tokens), F32),
        ),
        in_specs=[VMEM] * 3 + [ANY] * 6,
        out_specs=(VMEM, VMEM, VMEM),
        scratch_shapes=[
            vmem((tokens, width), F32),
            vmem((tokens, width), BF16),
            vmem((8, tokens), F32),
            vmem((n_t - 1, 8, tokens), F32),
            vmem((CORES, ff, unit), BF16),
            vmem((n_x, rows, cols), BF16),
            vmem((n_dp,) + proj.shape, BF16),
            vmem((n_dp, tokens, width), BF16),
            vmem((n_t, CORES, n_x, block, unit), BF16),
            vmem((CORES, n_x, block, unit), BF16),
            vmem(hops + (n_x * block, unit), BF16),
            vmem(hops + (n_x * block, unit), BF16),
            vmem((2, n_x * block, unit), F32),
            vmem((tokens, width), F32),
            vmem((tokens, 1), F32),
            vmem((8, tokens), F32),
            vmem((n_t - 1, 8, tokens), F32),
            sems((CORES,)),
            sems((n_x,)),
            sems((n_dp, 2)),
            sems(hops),
            sems(hops),
            sems((n_x,)),
            sems((n_x,)),
            sems((n_x,)),
            sems((n_x,)),
            sems((CORES, n_x)),
            sems((CORES, n_x)),
            sems(hops),
            sems(hops),
            sems((n_t - 1,)),
            sems((n_t - 1,)),
            sems((n_x,)),
            sems((n_x,)),
            sems((n_x,)),
            sems((n_x,)),
            sems(()),
            sems((n_t - 1,)),
            sems((n_t - 1,)),
        ],
        compiler_params=pltpu.CompilerParams(collective_id=2, has_side_effects=True, vmem_limit_bytes=GRANT),
        name="student",
    )(teacher_gain[None, :], dest_row[None, :], here, raw, hiddens, w_down, downs, proj, projs)


def local(
    attn_ctx,
    w_out,
    resid,
    teacher_gain,
    dest_row,
    student_in,
    student_gain,
    w_gate,
    w_up,
    w_down,
    proj,
):
    raw, hiddens, projs, downs, here = front(
        student_in, student_gain, attn_ctx, resid, w_gate, w_up, w_down, w_out, proj
    )
    out, residue, loss = student(raw, teacher_gain, dest_row, here, hiddens, w_down, downs, proj, projs)
    return (out, loss[0], residue)


def solution(mesh):
    placed = (
        P("dp", "tensor"),
        P("tensor", None),
        P(("dp", "tensor"), None),
        P(),
        P(),
        P("dp", "tensor"),
        P(),
        P("dp", "tensor"),
        P("dp", "tensor"),
        P("tensor", "dp"),
        P("dp", "tensor"),
    )
    return jax.shard_map(
        local,
        mesh=mesh,
        in_specs=placed,
        out_specs=(P("dp", "tensor"), P("dp"), P("dp", "tensor")),
        check_vma=False,
    )
```
